512 devices in a mesh: actors: 128 (over y, z, core), rep: 4 (over x).
Axes of the slice: x: 4, y: 8, z: 8, core: 2. Of those that a mesh axis runs over, the one named last changes fastest.
Arguments:
- features: bfloat16 [4, 128, 256, 1024], P('rep', 'actors'), may hold values from -6 to 6
- rewards: float32 [4, 128, 256], P('rep', 'actors'), may hold values from -2 to 6, as said below
- lengths: int32 [4, 128, 128], P('rep', 'actors'), may hold values from 1 to 3, 256 in all within a row
- owners: int32 [4, 128, 128], P('rep', 'actors'), may hold values from 0 to 127, each once within a row
- norm_gain: float32 [1024], replicated, may hold values from 0.4 to 1.6
Outputs:
- trainer_rows: bfloat16 [4, 128, 384, 1024], P('rep', 'actors')
- trainer_rewards: float32 [4, 128, 384], P('rep', 'actors')
- trainer_counts: int32 [128], P('actors')
The draws below stay inside these ranges and needn't reach their ends.
Inputs may be any that keep to these rules, and one draw needn't show every extreme that they name: `rewards`: rewards of each actor are centered on a level that differs from actor to actor.
All inputs are finite; a program needn't handle non-finite values.
Results may differ from the reference program's by a relative error of at most 0.0004.
Values may be sent and summed in bfloat16 or wider, within the bound.
A program may use at most 64 MiB of HBM per device.

```python
import math
import jax
import jax.numpy as jnp
import numpy as np
from jax import lax

F = 1024
GAMES = 128
ROWS_DEV = 256
CAP = 3
N_ACTORS = 128
N_REP = 4


def draw_rewards(key, part):
    shape = (N_REP, N_ACTORS, ROWS_DEV)
    device_pos = (jnp.arange(N_REP)[:, None, None] * N_ACTORS + jnp.arange(N_ACTORS)[None, :, None]).astype(jnp.float32)
    level = 1.0 + 2.0 * device_pos / (N_REP * N_ACTORS - 1)
    noise = jnp.clip(jax.random.normal(jax.random.fold_in(key, 3), shape, jnp.float32), -3.0, 3.0)
    return (level + noise).astype(jnp.float32)


def steps_of(key, extent, cuts, smallest, top_value):
    loudness, own = 1.0, jax.random.fold_in(key, 6)
    for axis_at, shards_of in cuts:
        steps = jnp.exp(jax.random.uniform(jax.random.fold_in(own, axis_at), (shards_of,), jnp.float32, smallest / len(cuts), top_value / len(cuts)))
        loudness = loudness * jnp.repeat(steps, extent[axis_at] // shards_of).reshape([-1 if axis == axis_at else 1 for axis in range(len(extent))])
    return loudness


def profile(number_of, total, reach, skew):
    weights = [(1 << 20) // math.isqrt(standing ** skew) + 1 for standing in range(2, number_of + 1)]
    spare, given = total - reach - (number_of - 1), [1] * (number_of - 1)
    while spare > 0:
        movable = [i for i in range(number_of - 1) if given[i] < reach]
        mass, budget = sum([weights[i] for i in movable]), spare
        for i in movable:
            addition = min(reach - given[i], max(1, budget * weights[i] // mass), spare)
            given[i] = given[i] + addition
            spare = spare - addition
    return np.array([reach] + given)


def uneven(stream_key, count, total, reach, slope):
    if count == 2:
        one = jax.random.randint(stream_key, (), max(1, total - reach), min(reach, total - 1) + 1)
        return jnp.stack([one, total - one])
    sizes = jnp.asarray(profile(count, total, reach, slope), jnp.int32)
    couples = (count - 1) // 2
    giver, receiver = sizes[1:1 + 2 * couples:2], sizes[2:2 + 2 * couples:2]
    slack = jnp.minimum(giver - 1, reach - receiver)
    shifted = jax.random.randint(jax.random.fold_in(stream_key, 1), (couples,), 0, 1 << 20) % (slack + 1)
    sizes = sizes.at[1:1 + 2 * couples:2].set(giver - shifted).at[2:2 + 2 * couples:2].set(receiver + shifted)
    return sizes[jax.random.permutation(jax.random.fold_in(stream_key, 2), count)]


def bell_draw(rng, extent, spread, most, cuts=(), kind=jnp.bfloat16):
    factor_of = steps_of(rng, extent, cuts, -0.22, 0.18) if cuts else 1.0
    values = jax.random.normal(rng, extent, jnp.float32) * spread * factor_of
    return jnp.minimum(jnp.maximum(values, -most), most).astype(kind)


def setup_inputs(seed: int = 0) -> dict:
    streams_of = jax.random.split(jax.random.key(seed), 6)
    features = bell_draw(streams_of[0], (N_REP, N_ACTORS, ROWS_DEV, F), 1.0, 6.0, ((0, 4), (1, 128)))
    rewards = draw_rewards(jax.random.fold_in(streams_of[5], 71), 0)
    lengths = jax.vmap(lambda own: uneven(own, GAMES, ROWS_DEV, CAP, 2))(jax.random.split(streams_of[2], N_REP * N_ACTORS)).reshape((N_REP, N_ACTORS, GAMES)).astype(jnp.int32)
    owners = jax.vmap(lambda own: jax.random.permutation(own, GAMES))(jax.random.split(streams_of[3], N_REP * N_ACTORS)).reshape((N_REP, N_ACTORS, GAMES)).astype(jnp.int32)
    norm_gain = jnp.clip(1.0 + 0.12 * jax.random.normal(streams_of[4], (F,), jnp.float32), 0.4, 1.6)
    return {"features": features, "rewards": rewards, "lengths": lengths, "owners": owners, "norm_gain": norm_gain}


EPS_NORM = 1e-06
EPS_VAR = 1e-05

def rms_scale(rows, norm_gain):
    widened = rows.astype(jnp.float32)
    square_mean = lax.optimization_barrier(jnp.mean(widened * widened, axis=-1, keepdims=True))
    return (widened * lax.rsqrt(square_mean + EPS_NORM) * norm_gain).astype(jnp.bfloat16)

def reference(features, rewards, lengths, owners, norm_gain):
    row_total = N_REP * N_ACTORS * ROWS_DEV
    reward_mean = jnp.sum(rewards) / row_total
    second = jnp.sum(rewards * rewards) / row_total
    inv_spread = lax.rsqrt(second - reward_mean * reward_mean + EPS_VAR)
    starts = jnp.cumsum(lengths, axis=-1) - lengths
    trainer_ids = jnp.arange(GAMES, dtype=jnp.int32)
    owns_game = (owners[..., None, :] == trainer_ids[:, None]).astype(jnp.int32)
    held_len = lax.optimization_barrier(jnp.sum(owns_game * lengths[..., None, :], axis=-1))
    held_start = lax.optimization_barrier(jnp.sum(owns_game * starts[..., None, :], axis=-1))
    slot_pos = jnp.arange(CAP, dtype=jnp.int32)
    usable = slot_pos < held_len[..., None]
    row_index = jnp.minimum(held_start[..., None] + slot_pos, ROWS_DEV - 1).astype(jnp.int32)
    scaled_rewards = (rewards - reward_mean) * inv_spread

    def one_group(group):
        group_feats, group_rews, group_index, group_keep = group
        normed = rms_scale(group_feats, norm_gain)
        picked = jax.vmap(lambda block_rows, picks: jnp.take(block_rows, picks, axis=0))(normed, group_index)
        picked = jnp.where(group_keep[..., None], picked, jnp.zeros((), jnp.bfloat16))
        picked_rew = jax.vmap(lambda block_rows, picks: jnp.take(block_rows, picks, axis=0))(group_rews, group_index)
        picked_rew = jnp.where(group_keep, picked_rew, jnp.zeros((), jnp.float32))
        rows_done = picked.transpose(1, 0, 2, 3).reshape(GAMES, GAMES * CAP, F)
        rews_done = picked_rew.transpose(1, 0, 2).reshape(GAMES, GAMES * CAP)
        return (rows_done, rews_done)
    rows_out, rews_out = lax.map(one_group, (features, scaled_rewards, row_index, usable))
    counts = lax.optimization_barrier(jnp.sum(held_len, axis=(0, 1))).astype(jnp.int32)
    return (rows_out, rews_out, counts)
```

```python
import functools

import jax
import jax.numpy as jnp
from jax import lax
from jax.experimental import pallas as pl
from jax.experimental.pallas import tpu as pltpu
from jax.sharding import PartitionSpec as P

CAP = 3
EPS_NORM = 1e-06
EPS_VAR = 1e-05
LANES = 128
VMEM = pl.BlockSpec(memory_space=pltpu.VMEM)
SMEM = pl.BlockSpec(memory_space=pltpu.SMEM)
MESH = pl.DeviceIdType.MESH


def pack_kernel(feats, rews, lens, owns, gain, packed, meta, wide):
    rows, width = feats.shape
    games = lens.shape[1]
    tiles = width // LANES
    length = lens[...].astype(jnp.float32)
    game = lax.broadcasted_iota(jnp.int32, (games, games), 1)
    trainer = lax.broadcasted_iota(jnp.int32, (games, games), 0)
    owned = owns[...] == trainer
    game_of = jnp.sum(jnp.where(owned, game, 0).astype(jnp.float32), axis=1, keepdims=True)
    held_len = jnp.sum(jnp.where(owned, length, 0.0), axis=1, keepdims=True)
    before = game.astype(jnp.float32) < game_of
    held_start = jnp.sum(jnp.where(before, length, 0.0), axis=1, keepdims=True)
    offset = lax.broadcasted_iota(jnp.int32, (games, rows), 1).astype(jnp.float32) - held_start
    usable = offset < held_len

    x = feats[...].astype(jnp.float32)
    square_mean = jnp.mean(x * x, axis=-1, keepdims=True)
    normed = (x * lax.rsqrt(square_mean + EPS_NORM) * gain[...]).astype(jnp.bfloat16)

    reward = rews[...]
    lane = lax.broadcasted_iota(jnp.int32, (games, LANES), 1)
    note = jnp.where(lane == CAP, held_len, 0.0)
    note = jnp.where(lane == CAP + 1, jnp.sum(reward), note)
    note = jnp.where(lane == CAP + 2, jnp.sum(reward * reward), note)
    for j in range(CAP):
        chosen = (offset == float(j)) & usable
        picked = jnp.dot(
            chosen.astype(jnp.float32).astype(jnp.bfloat16), normed, preferred_element_type=jnp.float32
        )
        for t in range(games // 8):
            for c in range(tiles):
                wide[pl.ds(t * 8 * CAP * tiles + j * tiles + c, 8, stride=CAP * tiles), :] = picked[
                    t * 8 : t * 8 + 8, c * LANES : (c + 1) * LANES
                ]
        held = jnp.sum(jnp.where(chosen, reward, 0.0), axis=1, keepdims=True)
        note = jnp.where(lane == j, held, note)
    packed[...] = wide[...].astype(jnp.bfloat16).reshape(packed.shape)
    meta[...] = note.reshape(meta.shape)


def send_kernel(n, n_rep, packed, meta, land, notes, totals, mine, others, m_send, m_recv, b_send, b_recv, s_send, s_recv):
    me = lax.axis_index("actors")
    rep = lax.axis_index("rep")
    barrier = pltpu.get_barrier_semaphore()

    @pl.loop(1, n)
    def _(k):
        pl.semaphore_signal(barrier, inc=1, device_id={"actors": lax.rem(me + k, n)}, device_id_type=MESH)

    for k in range(1, n_rep):
        pl.semaphore_signal(barrier, inc=1, device_id={"rep": lax.rem(rep + k, n_rep)}, device_id_type=MESH)
    pl.semaphore_wait(barrier, n - 1 + n_rep - 1)

    @pl.loop(1, n)
    def _(k):
        peer = lax.rem(me + k, n)
        pltpu.make_async_remote_copy(
            src_ref=meta.at[peer], dst_ref=notes.at[me], send_sem=m_send, recv_sem=m_recv,
            device_id={"actors": peer}, device_id_type=MESH,
        ).start()

    @pl.loop(1, n)
    def _(k):
        peer = lax.rem(me + k, n)
        pltpu.make_async_remote_copy(
            src_ref=packed.at[peer], dst_ref=land.at[me], send_sem=b_send, recv_sem=b_recv,
            device_id={"actors": peer}, device_id_type=MESH,
        ).start()

    notes[me] = meta[me]
    land[me] = packed[me]
    some = pl.ds(0, n - 1)
    pltpu.make_async_copy(notes.at[some], notes.at[some], m_recv).wait()
    total = jnp.sum(notes[...], axis=0)
    mine[...] = total
    copies = []
    for k in range(1, n_rep):
        copies.append(
            pltpu.make_async_remote_copy(
                src_ref=mine, dst_ref=others.at[n_rep - 1 - k], send_sem=s_send.at[k - 1], recv_sem=s_recv.at[n_rep - 1 - k],
                device_id={"rep": lax.rem(rep + k, n_rep)}, device_id_type=MESH,
            )
        )
        copies[-1].start()
    for k in range(n_rep - 1):
        pltpu.make_async_copy(others.at[k], others.at[k], s_recv.at[k]).wait()
    for k in range(n_rep - 1):
        total = total + others[k]
    totals[...] = total
    for copy in copies:
        copy.wait_send()
    pltpu.make_async_copy(notes.at[some], notes.at[some], m_send).wait()
    pltpu.make_async_copy(land.at[some], land.at[some], b_recv).wait()
    pltpu.make_async_copy(land.at[some], land.at[some], b_send).wait()


def unpack_kernel(row_total, land, notes, totals, rows, rews, counts, wide):
    games = land.shape[0]
    slots, width = rows.shape
    tiles = width // LANES
    wide[...] = land[...].reshape(wide.shape).astype(jnp.float32)
    for r in range(slots // 8):
        for c in range(tiles):
            rows[r * 8 : r * 8 + 8, c * LANES : (c + 1) * LANES] = wide[
                pl.ds(r * 8 * tiles + c, 8, stride=tiles), :
            ].astype(jnp.bfloat16)
    total = totals[...]
    counts[0] = jnp.sum(total[0:1, CAP : CAP + 1]).astype(jnp.int32)
    mean = total[0:1, CAP + 1 : CAP + 2] / row_total
    second = total[0:1, CAP + 2 : CAP + 3] / row_total
    spread = lax.rsqrt(second - mean * mean + EPS_VAR)
    note = notes[...]
    slot = lax.broadcasted_iota(jnp.int32, (games, slots), 1) - CAP * lax.broadcasted_iota(jnp.int32, (games, slots), 0)
    out = jnp.zeros((games, slots), jnp.float32)
    for j in range(CAP):
        held = (note[:, j : j + 1] - mean) * spread
        held = jnp.where(float(j) < note[:, CAP : CAP + 1], held, 0.0)
        out = out + jnp.where(slot == j, held, 0.0)
    rews[...] = jnp.sum(out, axis=0, keepdims=True)


def local(n, n_rep, features, rewards, lengths, owners, norm_gain):
    rows, width = features.shape[2:]
    games = lengths.shape[2]
    tiles = width // LANES
    message = (games, CAP * tiles, LANES)
    packed, meta = pl.pallas_call(
        pack_kernel,
        out_shape=(
            jax.ShapeDtypeStruct(message, jnp.bfloat16),
            jax.ShapeDtypeStruct((games, 1, LANES), jnp.float32),
        ),
        in_specs=[VMEM] * 5,
        out_specs=(VMEM, VMEM),
        scratch_shapes=[pltpu.VMEM((games * CAP * tiles, LANES), jnp.float32)],
        name="pack",
    )(features[0, 0], rewards[0], lengths[0], owners[0], norm_gain[None])
    land, notes, totals = pl.pallas_call(
        functools.partial(send_kernel, n, n_rep),
        out_shape=(
            jax.ShapeDtypeStruct(message, jnp.bfloat16),
            jax.ShapeDtypeStruct((games, 1, LANES), jnp.float32),
            jax.ShapeDtypeStruct((1, LANES), jnp.float32),
        ),
        in_specs=[VMEM] * 2,
        out_specs=(VMEM,) * 3,
        scratch_shapes=[
            pltpu.VMEM((1, LANES), jnp.float32),
            pltpu.VMEM((n_rep - 1, 1, LANES), jnp.float32),
            pltpu.SemaphoreType.DMA,
            pltpu.SemaphoreType.DMA,
            pltpu.SemaphoreType.DMA,
            pltpu.SemaphoreType.DMA,
            pltpu.SemaphoreType.DMA((n_rep - 1,)),
            pltpu.SemaphoreType.DMA((n_rep - 1,)),
        ],
        compiler_params=pltpu.CompilerParams(collective_id=0, has_side_effects=True),
        name="send",
    )(packed, meta)
    slots = games * CAP
    landed, scaled, counts = pl.pallas_call(
        functools.partial(unpack_kernel, float(rows * n * n_rep)),
        out_shape=(
            jax.ShapeDtypeStruct((slots, width), jnp.bfloat16),
            jax.ShapeDtypeStruct((1, slots), jnp.float32),
            jax.ShapeDtypeStruct((1,), jnp.int32),
        ),
        in_specs=[VMEM] * 3,
        out_specs=(VMEM, VMEM, SMEM),
        scratch_shapes=[pltpu.VMEM((slots * tiles, LANES), jnp.float32)],
        name="unpack",
    )(land, notes.reshape(games, LANES), totals)
    return landed.reshape(1, 1, slots, width), scaled.reshape(1, 1, slots), counts


def solution(mesh):
    n, n_rep = mesh.shape["actors"], mesh.shape["rep"]
    return jax.shard_map(
        functools.partial(local, n, n_rep),
        mesh=mesh,
        in_specs=(
            P("rep", "actors", None, None),
            P("rep", "actors", None),
            P("rep", "actors", None),
            P("rep", "actors", None),
            P(),
        ),
        out_specs=(P("rep", "actors", None, None), P("rep", "actors", None), P("actors")),
        check_vma=False,
    )
```

```python
import functools

import jax
import jax.numpy as jnp
from jax import lax
from jax.experimental import pallas as pl
from jax.experimental.pallas import tpu as pltpu
from jax.sharding import PartitionSpec as P

CAP = 3
EPS_NORM = 1e-06
EPS_VAR = 1e-05
LANES = 128
SIDE = 8
FIELDS = 16
ORDER = (0, 4, 5, 3, 6, 2, 7, 1)
GROUPS = ((0, 4), (4, 4))
VMEM = pl.BlockSpec(memory_space=pltpu.VMEM)
SMEM = pl.BlockSpec(memory_space=pltpu.SMEM)
HBM = pl.BlockSpec(memory_space=pltpu.HBM)
MESH = pl.DeviceIdType.MESH


def place():
    me = lax.axis_index("actors")
    return me // (2 * SIDE), lax.rem(me // 2, SIDE), lax.rem(me, 2)


def actor(y, z, c):
    return (lax.rem(y, SIDE) * SIDE + lax.rem(z, SIDE)) * 2 + lax.rem(c, 2)


def distance(k):
    out = jnp.zeros_like(k)
    for i, d in enumerate(ORDER):
        out = jnp.where(k == i, d, out)
    return out


def wait(sem, ref):
    pltpu.make_async_copy(ref, ref, sem).wait()


def route_kernel(
    n_rep, row_total, feats_in, rews_in, lens_in, owns_in, gain_in, spread_rows, spread_rews, counts,
    feats, rews, lens, owns, gain, wide, packed, via_z, via_y, land_z, land_y,
    note_z, note_c, notes1, notes2, mine, others,
    in_sem, a_send, b_send, a_recv, b_recv, a2_send, b2_send, a2_recv, b2_recv,
    n1_send, n1_recv, n2_send, n2_recv, s_send, s_recv,
):
    y, z, c = place()
    rep = lax.axis_index("rep")
    tiles = feats.shape[1] // LANES
    piece = CAP * tiles
    rows = feats.shape[0]
    games = lens.shape[1]

    inputs = [
        pltpu.make_async_copy(src, dst, in_sem.at[i])
        for i, (src, dst) in enumerate(
            ((feats_in, feats), (rews_in, rews), (lens_in, lens), (owns_in, owns), (gain_in, gain))
        )
    ]
    for copy in inputs:
        copy.start()
    barrier = pltpu.get_barrier_semaphore()
    for d in ORDER[1:]:
        for peer in (actor(y, z + d, c), actor(y + d, z, c), actor(y, z + d, c + 1)):
            pl.semaphore_signal(barrier, inc=1, device_id={"actors": peer}, device_id_type=MESH)
    pl.semaphore_signal(barrier, inc=1, device_id={"actors": actor(y, z, c + 1)}, device_id_type=MESH)
    for k in range(1, n_rep):
        pl.semaphore_signal(barrier, inc=1, device_id={"rep": lax.rem(rep + k, n_rep)}, device_id_type=MESH)
    for copy in inputs[1:]:
        copy.wait()

    row = lax.broadcasted_iota(jnp.int32, (games, 1), 0)
    inner = row & (SIDE - 1)
    step = distance((row // SIDE) & (SIDE - 1))
    near = row < games // 2
    to_y = jnp.where(near, inner, (y + step) & (SIDE - 1))
    to_z = jnp.where(near, (z + step) & (SIDE - 1), inner)
    trainer = (to_y * SIDE + to_z) * 2 + jnp.where(near, c, 1 - c)
    length = lens[...].astype(jnp.float32)
    game = lax.broadcasted_iota(jnp.int32, (games, games), 1).astype(jnp.float32)
    owned = owns[...] == trainer
    game_of = jnp.sum(jnp.where(owned, game, 0.0), axis=1, keepdims=True)
    held_len = jnp.sum(jnp.where(owned, length, 0.0), axis=1, keepdims=True)
    held_start = jnp.sum(jnp.where(game < game_of, length, 0.0), axis=1, keepdims=True)
    offset = lax.broadcasted_iota(jnp.int32, (games, rows), 1).astype(jnp.float32) - held_start
    usable = offset < held_len

    reward = rews[...]
    lane = lax.broadcasted_iota(jnp.int32, (games, LANES), 1) - to_y * FIELDS
    note = jnp.where(lane == CAP, held_len, 0.0)
    note = jnp.where(lane == CAP + 1, jnp.sum(reward), note)
    note = jnp.where(lane == CAP + 2, jnp.sum(reward * reward), note)
    chosen = []
    for j in range(CAP):
        chosen.append((offset == float(j)) & usable)
        held = jnp.sum(jnp.where(chosen[j], reward, 0.0), axis=1, keepdims=True)
        note = jnp.where(lane == j, held, note)
    crossing = jnp.zeros((SIDE, LANES), jnp.float32)
    for k in range(SIDE):
        note_z[k] = jnp.sum(note[k * SIDE : (k + 1) * SIDE], axis=0, keepdims=True)
        crossing = crossing + note[games // 2 + k * SIDE : games // 2 + (k + 1) * SIDE]
    note_c[...] = crossing.reshape(note_c.shape)

    inputs[0].wait()
    x = feats[...].astype(jnp.float32)
    square_mean = jnp.mean(x * x, axis=-1, keepdims=True)
    normed = (x * lax.rsqrt(square_mean + EPS_NORM) * gain[...]).astype(jnp.bfloat16)
    for j in range(CAP):
        picked = jnp.dot(
            chosen[j].astype(jnp.float32).astype(jnp.bfloat16), normed, preferred_element_type=jnp.float32
        )
        for t in range(games // 8):
            for q in range(tiles):
                wide[pl.ds(t * 8 * piece + j * tiles + q, 8, stride=piece), :] = picked[
                    t * 8 : t * 8 + 8, q * LANES : (q + 1) * LANES
                ]
    packed[...] = wide[...].astype(jnp.bfloat16).reshape(packed.shape)
    via_z[0] = packed[0, 0]
    via_y[0] = packed[1, 0]
    notes1[0] = note_z[0]

    pl.semaphore_wait(barrier, 3 * SIDE - 2 + n_rep - 1)

    def send(src, dst, send_sem, recv_sem, peer):
        pltpu.make_async_remote_copy(
            src_ref=src, dst_ref=dst, send_sem=send_sem, recv_sem=recv_sem, device_id=peer, device_id_type=MESH
        ).start()

    for k in range(SIDE):
        d = ORDER[k]
        if k:
            send(note_z.at[k], notes1.at[k], n1_send, n1_recv, {"actors": actor(y, z + d, c)})
        send(
            note_c.at[lax.rem(z + d, SIDE)], notes1.at[SIDE + k], n1_send, n1_recv,
            {"actors": actor(y, z + d, c + 1)},
        )
    for k in range(1, SIDE):
        d = ORDER[k]
        send(packed.at[0, k], via_z.at[k], a_send, a_recv.at[k], {"actors": actor(y, z + d, c)})
        send(packed.at[1, k], via_y.at[k], b_send, b_recv.at[k], {"actors": actor(y + d, z, c)})

    wait(n1_recv, notes1.at[pl.ds(1, 2 * SIDE - 1)])
    for k in range(1, SIDE):
        send(notes1, notes2.at[k], n2_send, n2_recv, {"actors": actor(y + ORDER[k], z, c)})
    notes2[0] = notes1[...]

    for g, (low, count) in enumerate(GROUPS):
        some = pl.ds(low, count)
        for k in range(max(low, 1), low + count):
            wait(a_recv.at[k], via_z.at[k])
        for k in range(1, SIDE):
            d = ORDER[k]
            send(
                via_z.at[some, lax.rem(y + d, SIDE)], land_z.at[k, some], a2_send, a2_recv.at[k, g],
                {"actors": actor(y + d, z, c)},
            )
        for k in range(max(low, 1), low + count):
            wait(b_recv.at[k], via_y.at[k])
        for k in range(SIDE):
            d = ORDER[k]
            send(
                via_y.at[some, lax.rem(z + d, SIDE)], land_y.at[k, some], b2_send, b2_recv.at[k, g],
                {"actors": actor(y, z + d, c + 1)},
            )

    wait(n2_recv, notes2.at[pl.ds(1, SIDE - 1)])
    arrived = notes2[...].reshape(games, LANES)
    total = jnp.sum(arrived, axis=0, keepdims=True)
    mine[...] = total
    for k in range(1, n_rep):
        send(mine, others.at[k - 1], s_send.at[k - 1], s_recv.at[k - 1], {"rep": lax.rem(rep + k, n_rep)})

    def widen(value, ky, kz, core):
        source = actor(y + SIDE - ORDER[ky], z + SIDE - ORDER[kz], core)
        spread_rows[pl.ds(pl.multiple_of(source * piece, 8), piece), :] = value.astype(jnp.float32)

    for k in range(SIDE):
        widen(via_z[k, y], 0, k, c)

    for k in range(1, n_rep):
        wait(s_recv.at[k - 1], others.at[k - 1])
    for k in range(1, n_rep):
        total = total + others[k - 1]
    row_lane = lax.broadcasted_iota(jnp.int32, (1, LANES), 1) - y * FIELDS

    def field(i):
        return jnp.sum(jnp.where(row_lane == i, total, 0.0), axis=1, keepdims=True)

    counts[...] = jnp.broadcast_to(field(CAP), counts.shape).astype(jnp.int32)
    mean = field(CAP + 1) / row_total
    spread = lax.rsqrt(field(CAP + 2) / row_total - mean * mean + EPS_VAR)
    from_y = (y + SIDE - distance(row // (2 * SIDE))) & (SIDE - 1)
    from_z = (z + SIDE - distance(inner)) & (SIDE - 1)
    source = (from_y * SIDE + from_z) * 2 + jnp.where((row & SIDE) == 0, c, 1 - c)
    slots = games * CAP
    slot = lax.broadcasted_iota(jnp.int32, (games, slots), 1) - CAP * source
    lane = lax.broadcasted_iota(jnp.int32, (games, LANES), 1) - y * FIELDS

    def column(i):
        return jnp.sum(jnp.where(lane == i, arrived, 0.0), axis=1, keepdims=True)

    held_len = column(CAP)
    out = jnp.zeros((games, slots), jnp.float32)
    for j in range(CAP):
        value = jnp.where(float(j) < held_len, (column(j) - mean) * spread, 0.0)
        out = out + jnp.where(slot == j, value, 0.0)
    spread_rews[...] = jnp.sum(out, axis=0, keepdims=True)

    for g, (low, count) in enumerate(GROUPS):
        some = pl.ds(low, count)
        for k in range(SIDE):
            if k:
                wait(a2_recv.at[k, g], land_z.at[k, some])
                for i in range(low, low + count):
                    widen(land_z[k, i], k, i, c)
            wait(b2_recv.at[k, g], land_y.at[k, some])
            for i in range(low, low + count):
                widen(land_y[k, i], i, k, c + 1)

    rest = pl.ds(1, SIDE - 1)
    wait(n1_send, notes1.at[pl.ds(1, 2 * SIDE - 1)])
    wait(n2_send, notes2.at[rest])
    for k in range(1, n_rep):
        wait(s_send.at[k - 1], others.at[k - 1])
    wait(a_send, via_z.at[rest])
    wait(b_send, via_y.at[rest])
    wait(a2_send, land_z.at[rest])
    wait(b2_send, land_y)


def write_kernel(spread_rows, spread_rews, count, rows, rews, counts):
    tiles = rows.shape[1] // LANES
    for r in range(rows.shape[0] // 8):
        for q in range(tiles):
            rows[r * 8 : r * 8 + 8, q * LANES : (q + 1) * LANES] = spread_rows[
                pl.ds(r * 8 * tiles + q, 8, stride=tiles), :
            ].astype(jnp.bfloat16)
    rews[...] = spread_rews[...]
    counts[0] = jnp.max(count[...])


def local(n, n_rep, features, rewards, lengths, owners, norm_gain):
    rows, width = features.shape[2:]
    games = lengths.shape[2]
    piece = CAP * width // LANES
    slots = games * CAP
    DMA = pltpu.SemaphoreType.DMA
    block = pltpu.VMEM((SIDE, SIDE, piece, LANES), jnp.bfloat16)
    spread_rows, spread_rews, count = pl.pallas_call(
        functools.partial(route_kernel, n_rep, float(rows * n * n_rep)),
        out_shape=(
            jax.ShapeDtypeStruct((games * piece, LANES), jnp.float32),
            jax.ShapeDtypeStruct((1, slots), jnp.float32),
            jax.ShapeDtypeStruct((1, LANES), jnp.int32),
        ),
        in_specs=[HBM] * 5,
        out_specs=(VMEM,) * 3,
        scratch_shapes=[
            pltpu.VMEM((rows, width), jnp.bfloat16),
            pltpu.VMEM((1, rows), jnp.float32),
            pltpu.VMEM((1, games), jnp.int32),
            pltpu.VMEM((1, games), jnp.int32),
            pltpu.VMEM((1, width), jnp.float32),
            pltpu.VMEM((games * piece, LANES), jnp.float32),
            pltpu.VMEM((2, SIDE, SIDE, piece, LANES), jnp.bfloat16),
            block,
            block,
            block,
            block,
            pltpu.VMEM((SIDE, 1, LANES), jnp.float32),
            pltpu.VMEM((SIDE, 1, LANES), jnp.float32),
            pltpu.VMEM((2 * SIDE, 1, LANES), jnp.float32),
            pltpu.VMEM((SIDE, 2 * SIDE, 1, LANES), jnp.float32),
            pltpu.VMEM((1, LANES), jnp.float32),
            pltpu.VMEM((n_rep - 1, 1, LANES), jnp.float32),
            DMA((5,)),
            DMA,
            DMA,
            DMA((SIDE,)),
            DMA((SIDE,)),
            DMA,
            DMA,
            DMA((SIDE, len(GROUPS))),
            DMA((SIDE, len(GROUPS))),
            DMA,
            DMA,
            DMA,
            DMA,
            DMA((n_rep - 1,)),
            DMA((n_rep - 1,)),
        ],
        compiler_params=pltpu.CompilerParams(
            collective_id=0, has_side_effects=True, vmem_limit_bytes=24 * 1024 * 1024
        ),
        name="route",
    )(features[0, 0], rewards[0], lengths[0], owners[0], norm_gain[None])
    landed, scaled, counts = pl.pallas_call(
        write_kernel,
        out_shape=(
            jax.ShapeDtypeStruct((slots, width), jnp.bfloat16),
            jax.ShapeDtypeStruct((1, slots), jnp.float32),
            jax.ShapeDtypeStruct((1,), jnp.int32),
        ),
        in_specs=[VMEM] * 3,
        out_specs=(VMEM, VMEM, SMEM),
        compiler_params=pltpu.CompilerParams(vmem_limit_bytes=24 * 1024 * 1024),
        name="write",
    )(spread_rows, spread_rews, count)
    return landed.reshape(1, 1, slots, width), scaled.reshape(1, 1, slots), counts


def solution(mesh):
    n, n_rep = mesh.shape["actors"], mesh.shape["rep"]
    return jax.shard_map(
        functools.partial(local, n, n_rep),
        mesh=mesh,
        in_specs=(
            P("rep", "actors", None, None),
            P("rep", "actors", None),
            P("rep", "actors", None),
            P("rep", "actors", None),
            P(),
        ),
        out_specs=(P("rep", "actors", None, None), P("rep", "actors", None), P("actors")),
        check_vma=False,
    )
```

```python
import functools

import jax
import jax.numpy as jnp
from jax import lax
from jax.experimental import pallas as pl
from jax.experimental.pallas import tpu as pltpu
from jax.sharding import PartitionSpec as P

CAP = 3
EPS_NORM = 1e-06
EPS_VAR = 1e-05
LANES = 128
SIDE = 8
FIELDS = 8
ORDER = (0, 4, 5, 3, 6, 2, 7, 1)
GROUPS = ((0, 4), (4, 4))
VMEM = pl.BlockSpec(memory_space=pltpu.VMEM)
SMEM = pl.BlockSpec(memory_space=pltpu.SMEM)
HBM = pl.BlockSpec(memory_space=pltpu.HBM)
MESH = pl.DeviceIdType.MESH


def place():
    me = lax.axis_index("actors")
    return me // (2 * SIDE), lax.rem(me // 2, SIDE), lax.rem(me, 2)


def actor(y, z, c):
    return (lax.rem(y, SIDE) * SIDE + lax.rem(z, SIDE)) * 2 + lax.rem(c, 2)


def distance(k):
    out = jnp.zeros_like(k)
    for i, d in enumerate(ORDER):
        out = jnp.where(k == i, d, out)
    return out


def wait(sem, ref):
    pltpu.make_async_copy(ref, ref, sem).wait()


def route_kernel(
    n_rep, row_total, feats_in, rews_in, lens_in, owns_in, gain_in, spread_rows, spread_rews, counts,
    feats, rews, lens, owns, gain, wide, packed, via_z, via_y, land_z, land_y,
    note_z, note_c, notes1, notes2, mine, others,
    in_sem, a_send, b_send, a_recv, b_recv, a2_send, b2_send, a2_recv, b2_recv,
    n1_send, n1_recv, n2_send, n2_recv, s_send, s_recv,
):
    y, z, c = place()
    rep = lax.axis_index("rep")
    tiles = feats.shape[1] // LANES
    piece = CAP * tiles
    rows = feats.shape[0]
    games = lens.shape[1]

    inputs = [
        pltpu.make_async_copy(src, dst, in_sem.at[i])
        for i, (src, dst) in enumerate(
            ((feats_in, feats), (rews_in, rews), (lens_in, lens), (owns_in, owns), (gain_in, gain))
        )
    ]
    for copy in inputs:
        copy.start()
    barrier = pltpu.get_barrier_semaphore()
    for d in ORDER[1:]:
        for peer in (actor(y, z + d, c), actor(y + d, z, c), actor(y, z + d, c + 1)):
            pl.semaphore_signal(barrier, inc=1, device_id={"actors": peer}, device_id_type=MESH)
    pl.semaphore_signal(barrier, inc=1, device_id={"actors": actor(y, z, c + 1)}, device_id_type=MESH)
    for k in range(1, n_rep):
        pl.semaphore_signal(barrier, inc=1, device_id={"rep": lax.rem(rep + k, n_rep)}, device_id_type=MESH)
    for copy in inputs[1:]:
        copy.wait()

    row = lax.broadcasted_iota(jnp.int32, (games, 1), 0)
    inner = row & (SIDE - 1)
    step = distance((row // SIDE) & (SIDE - 1))
    near = row < games // 2
    to_y = jnp.where(near, inner, (y + step) & (SIDE - 1))
    to_z = jnp.where(near, (z + step) & (SIDE - 1), inner)
    trainer = (to_y * SIDE + to_z) * 2 + jnp.where(near, c, 1 - c)
    length = lens[...].astype(jnp.float32)
    game = lax.broadcasted_iota(jnp.int32, (games, games), 1).astype(jnp.float32)
    owned = owns[...] == trainer
    game_of = jnp.sum(jnp.where(owned, game, 0.0), axis=1, keepdims=True)
    held_len = jnp.sum(jnp.where(owned, length, 0.0), axis=1, keepdims=True)
    held_start = jnp.sum(jnp.where(game < game_of, length, 0.0), axis=1, keepdims=True)
    offset = lax.broadcasted_iota(jnp.int32, (games, rows), 1).astype(jnp.float32) - held_start
    usable = offset < held_len

    reward = rews[...]
    half = SIDE * FIELDS
    lane = lax.broadcasted_iota(jnp.int32, (games, LANES), 1) - to_y * FIELDS - jnp.where(near, 0, half)
    note = jnp.where(lane == CAP, held_len, 0.0)
    note = jnp.where(lane == CAP + 1, jnp.sum(reward), note)
    note = jnp.where(lane == CAP + 2, jnp.sum(reward * reward), note)
    chosen = []
    for j in range(CAP):
        chosen.append((offset == float(j)) & usable)
        held = jnp.sum(jnp.where(chosen[j], reward, 0.0), axis=1, keepdims=True)
        note = jnp.where(lane == j, held, note)
    crossing = jnp.zeros((SIDE, LANES), jnp.float32)
    for k in range(SIDE):
        note_z[k] = jnp.sum(note[k * SIDE : (k + 1) * SIDE], axis=0, keepdims=True)
        crossing = crossing + note[games // 2 + k * SIDE : games // 2 + (k + 1) * SIDE]
    note_c[...] = crossing.reshape(note_c.shape)

    inputs[0].wait()
    x = feats[...].astype(jnp.float32)
    square_mean = jnp.mean(x * x, axis=-1, keepdims=True)
    normed = (x * lax.rsqrt(square_mean + EPS_NORM) * gain[...]).astype(jnp.bfloat16)
    for j in range(CAP):
        picked = jnp.dot(
            chosen[j].astype(jnp.float32).astype(jnp.bfloat16), normed, preferred_element_type=jnp.float32
        )
        for t in range(games // 8):
            for q in range(tiles):
                wide[pl.ds(t * 8 * piece + j * tiles + q, 8, stride=piece), :] = picked[
                    t * 8 : t * 8 + 8, q * LANES : (q + 1) * LANES
                ]
    packed[...] = wide[...].astype(jnp.bfloat16).reshape(packed.shape)
    via_z[0] = packed[0, 0]
    via_y[0] = packed[1, 0]
    notes1[0] = note_z[0]

    pl.semaphore_wait(barrier, 3 * SIDE - 2 + n_rep - 1)

    def send(src, dst, send_sem, recv_sem, peer):
        pltpu.make_async_remote_copy(
            src_ref=src, dst_ref=dst, send_sem=send_sem, recv_sem=recv_sem, device_id=peer, device_id_type=MESH
        ).start()

    for k in range(SIDE):
        d = ORDER[k]
        if k:
            send(note_z.at[k], notes1.at[k], n1_send, n1_recv, {"actors": actor(y, z + d, c)})
        send(
            note_c.at[lax.rem(z + d, SIDE)], notes1.at[SIDE + k], n1_send, n1_recv,
            {"actors": actor(y, z + d, c + 1)},
        )
    for k in range(1, SIDE):
        d = ORDER[k]
        send(packed.at[0, k], via_z.at[k], a_send, a_recv.at[k], {"actors": actor(y, z + d, c)})
        send(packed.at[1, k], via_y.at[k], b_send, b_recv.at[k], {"actors": actor(y + d, z, c)})

    wait(n1_recv, notes1.at[pl.ds(1, 2 * SIDE - 1)])
    notes2[0] = notes1[0:SIDE] + notes1[SIDE:]
    for k in range(1, SIDE):
        send(notes2.at[0], notes2.at[k], n2_send, n2_recv, {"actors": actor(y + ORDER[k], z, c)})

    for g, (low, count) in enumerate(GROUPS):
        some = pl.ds(low, count)
        for k in range(max(low, 1), low + count):
            wait(a_recv.at[k], via_z.at[k])
        for k in range(1, SIDE):
            d = ORDER[k]
            send(
                via_z.at[some, lax.rem(y + d, SIDE)], land_z.at[k, some], a2_send, a2_recv.at[k, g],
                {"actors": actor(y + d, z, c)},
            )
        for k in range(max(low, 1), low + count):
            wait(b_recv.at[k], via_y.at[k])
        for k in range(SIDE):
            d = ORDER[k]
            send(
                via_y.at[some, lax.rem(z + d, SIDE)], land_y.at[k, some], b2_send, b2_recv.at[k, g],
                {"actors": actor(y, z + d, c + 1)},
            )

    wait(n2_recv, notes2.at[pl.ds(1, SIDE - 1)])
    arrived = notes2[...].reshape(SIDE * SIDE, LANES)
    total = jnp.sum(arrived, axis=0, keepdims=True)
    mine[...] = total
    for k in range(1, n_rep):
        send(mine, others.at[k - 1], s_send.at[k - 1], s_recv.at[k - 1], {"rep": lax.rem(rep + k, n_rep)})

    def widen(value, ky, kz, core):
        source = actor(y + SIDE - ORDER[ky], z + SIDE - ORDER[kz], core)
        spread_rows[pl.ds(pl.multiple_of(source * piece, 8), piece), :] = value.astype(jnp.float32)

    for k in range(SIDE):
        widen(via_z[k, y], 0, k, c)

    for k in range(1, n_rep):
        wait(s_recv.at[k - 1], others.at[k - 1])
    for k in range(1, n_rep):
        total = total + others[k - 1]
    row_lane = lax.broadcasted_iota(jnp.int32, (1, LANES), 1) - y * FIELDS

    def field(i):
        return jnp.sum(jnp.where((row_lane == i) | (row_lane == i + half), total, 0.0), axis=1, keepdims=True)

    counts[...] = jnp.broadcast_to(field(CAP), counts.shape).astype(jnp.int32)
    mean = field(CAP + 1) / row_total
    spread = lax.rsqrt(field(CAP + 2) / row_total - mean * mean + EPS_VAR)
    pair = lax.broadcasted_iota(jnp.int32, (SIDE * SIDE, 1), 0)
    from_y = (y + SIDE - distance(pair // SIDE)) & (SIDE - 1)
    from_z = (z + SIDE - distance(pair & (SIDE - 1))) & (SIDE - 1)
    slots = games * CAP
    lane = lax.broadcasted_iota(jnp.int32, (SIDE * SIDE, LANES), 1) - y * FIELDS

    def column(i):
        return jnp.sum(jnp.where(lane == i, arrived, 0.0), axis=1, keepdims=True)

    out = jnp.zeros((SIDE * SIDE, slots), jnp.float32)
    for h in range(2):
        source = (from_y * SIDE + from_z) * 2 + jnp.where(h == c, 0, 1)
        slot = lax.broadcasted_iota(jnp.int32, (SIDE * SIDE, slots), 1) - CAP * source
        held_len = column(h * half + CAP)
        for j in range(CAP):
            value = jnp.where(float(j) < held_len, (column(h * half + j) - mean) * spread, 0.0)
            out = out + jnp.where(slot == j, value, 0.0)
    spread_rews[...] = jnp.sum(out, axis=0, keepdims=True)

    for g, (low, count) in enumerate(GROUPS):
        some = pl.ds(low, count)
        for k in range(SIDE):
            if k:
                wait(a2_recv.at[k, g], land_z.at[k, some])
                for i in range(low, low + count):
                    widen(land_z[k, i], k, i, c)
            wait(b2_recv.at[k, g], land_y.at[k, some])
            for i in range(low, low + count):
                widen(land_y[k, i], i, k, c + 1)

    rest = pl.ds(1, SIDE - 1)
    wait(n1_send, notes1.at[pl.ds(1, 2 * SIDE - 1)])
    wait(n2_send, notes2.at[rest])
    for k in range(1, n_rep):
        wait(s_send.at[k - 1], others.at[k - 1])
    wait(a_send, via_z.at[rest])
    wait(b_send, via_y.at[rest])
    wait(a2_send, land_z.at[rest])
    wait(b2_send, land_y)


def write_kernel(spread_rows, spread_rews, count, rows, rews, counts):
    tiles = rows.shape[1] // LANES
    for r in range(rows.shape[0] // 8):
        for q in range(tiles):
            rows[r * 8 : r * 8 + 8, q * LANES : (q + 1) * LANES] = spread_rows[
                pl.ds(r * 8 * tiles + q, 8, stride=tiles), :
            ].astype(jnp.bfloat16)
    rews[...] = spread_rews[...]
    counts[0] = jnp.max(count[...])


def local(n, n_rep, features, rewards, lengths, owners, norm_gain):
    rows, width = features.shape[2:]
    games = lengths.shape[2]
    piece = CAP * width // LANES
    slots = games * CAP
    DMA = pltpu.SemaphoreType.DMA
    inputs = (features[0, 0], rewards[0], lengths[0], owners[0], norm_gain[None])
    block = pltpu.VMEM((SIDE, SIDE, piece, LANES), jnp.bfloat16)
    spread_rows, spread_rews, count = pl.pallas_call(
        functools.partial(route_kernel, n_rep, float(rows * n * n_rep)),
        out_shape=(
            jax.ShapeDtypeStruct((games * piece, LANES), jnp.float32),
            jax.ShapeDtypeStruct((1, slots), jnp.float32),
            jax.ShapeDtypeStruct((1, LANES), jnp.int32),
        ),
        in_specs=[HBM] * 5,
        out_specs=(VMEM,) * 3,
        scratch_shapes=[
            pltpu.VMEM((rows, width), jnp.bfloat16),
            pltpu.VMEM((1, rows), jnp.float32),
            pltpu.VMEM((1, games), jnp.int32),
            pltpu.VMEM((1, games), jnp.int32),
            pltpu.VMEM((1, width), jnp.float32),
            pltpu.VMEM((games * piece, LANES), jnp.float32),
            pltpu.VMEM((2, SIDE, SIDE, piece, LANES), jnp.bfloat16),
            block,
            block,
            block,
            block,
            pltpu.VMEM((SIDE, 1, LANES), jnp.float32),
            pltpu.VMEM((SIDE, 1, LANES), jnp.float32),
            pltpu.VMEM((2 * SIDE, 1, LANES), jnp.float32),
            pltpu.VMEM((SIDE, SIDE, 1, LANES), jnp.float32),
            pltpu.VMEM((1, LANES), jnp.float32),
            pltpu.VMEM((n_rep - 1, 1, LANES), jnp.float32),
            DMA((5,)),
            DMA,
            DMA,
            DMA((SIDE,)),
            DMA((SIDE,)),
            DMA,
            DMA,
            DMA((SIDE, len(GROUPS))),
            DMA((SIDE, len(GROUPS))),
            DMA,
            DMA,
            DMA,
            DMA,
            DMA((n_rep - 1,)),
            DMA((n_rep - 1,)),
        ],
        compiler_params=pltpu.CompilerParams(
            collective_id=0, has_side_effects=True, vmem_limit_bytes=24 * 1024 * 1024
        ),
        name="route",
    )(*(pltpu.with_memory_space_constraint(a, pltpu.HBM) for a in inputs))
    landed, scaled, counts = pl.pallas_call(
        write_kernel,
        out_shape=(
            jax.ShapeDtypeStruct((slots, width), jnp.bfloat16),
            jax.ShapeDtypeStruct((1, slots), jnp.float32),
            jax.ShapeDtypeStruct((1,), jnp.int32),
        ),
        in_specs=[VMEM] * 3,
        out_specs=(VMEM, VMEM, SMEM),
        compiler_params=pltpu.CompilerParams(vmem_limit_bytes=24 * 1024 * 1024),
        name="write",
    )(spread_rows, spread_rews, count)
    return landed.reshape(1, 1, slots, width), scaled.reshape(1, 1, slots), counts


def solution(mesh):
    n, n_rep = mesh.shape["actors"], mesh.shape["rep"]
    return jax.shard_map(
        functools.partial(local, n, n_rep),
        mesh=mesh,
        in_specs=(
            P("rep", "actors", None, None),
            P("rep", "actors", None),
            P("rep", "actors", None),
            P("rep", "actors", None),
            P(),
        ),
        out_specs=(P("rep", "actors", None, None), P("rep", "actors", None), P("actors")),
        check_vma=False,
    )
```

```python
import functools

import jax
import jax.numpy as jnp
from jax import lax
from jax.experimental import pallas as pl
from jax.experimental.pallas import tpu as pltpu
from jax.sharding import PartitionSpec as P

CAP = 3
EPS_NORM = 1e-06
EPS_VAR = 1e-05
LANES = 128
SIDE = 8
FIELDS = 8
Z_ORDER = (0, 1, 2, 3, 4, 5, 6, 7)
Y_ORDER = (0, 1, 2, 3, 7, 6, 5, 4)
STEPS = (('y', (0, 8), (0, 8)), ('z', (0, 8), (0, 8)))
VMEM = pl.BlockSpec(memory_space=pltpu.VMEM)
SMEM = pl.BlockSpec(memory_space=pltpu.SMEM)
HBM = pl.BlockSpec(memory_space=pltpu.HBM)
MESH = pl.DeviceIdType.MESH


def place():
    me = lax.axis_index("actors")
    return me // (2 * SIDE), lax.rem(me // 2, SIDE), lax.rem(me, 2)


def actor(y, z, c):
    return (lax.rem(y, SIDE) * SIDE + lax.rem(z, SIDE)) * 2 + lax.rem(c, 2)


def wait(sem, ref):
    pltpu.make_async_copy(ref, ref, sem).wait()


def route_kernel(
    n_rep, row_total, feats_in, rews_in, lens_in, owns_in, gain_in, spread_rows, spread_rews, counts,
    feats, rews, lens, owns, gain, wide, packed, via_z, via_y, land_z, land_y,
    note_z, note_c, notes1, notes2, mine, others,
    in_sem, a_send, b_send, a_recv, b_recv, a2_send, b2_send, a2_recv, b2_recv,
    n1_send, n1_recv, n2_send, n2_recv, s_send, s_recv,
):
    y, z, c = place()
    rep = lax.axis_index("rep")
    tiles = feats.shape[1] // LANES
    piece = CAP * tiles
    rows = feats.shape[0]
    games = lens.shape[1]

    inputs = [
        pltpu.make_async_copy(src, dst, in_sem.at[i])
        for i, (src, dst) in enumerate(
            ((feats_in, feats), (rews_in, rews), (lens_in, lens), (owns_in, owns), (gain_in, gain))
        )
    ]
    for copy in inputs:
        copy.start()
    barrier = pltpu.get_barrier_semaphore()
    for d in range(1, SIDE):
        for peer in (actor(y, z + d, c), actor(y + d, z, c), actor(y, z + d, c + 1)):
            pl.semaphore_signal(barrier, inc=1, device_id={"actors": peer}, device_id_type=MESH)
    pl.semaphore_signal(barrier, inc=1, device_id={"actors": actor(y, z, c + 1)}, device_id_type=MESH)
    for k in range(1, n_rep):
        pl.semaphore_signal(barrier, inc=1, device_id={"rep": lax.rem(rep + k, n_rep)}, device_id_type=MESH)
    for copy in inputs[1:]:
        copy.wait()

    row = lax.broadcasted_iota(jnp.int32, (games, 1), 0)
    inner = row & (SIDE - 1)
    step = (row // SIDE) & (SIDE - 1)
    near = row < games // 2
    to_y = jnp.where(near, inner, step)
    to_z = jnp.where(near, step, inner)
    trainer = (to_y * SIDE + to_z) * 2 + jnp.where(near, c, 1 - c)
    length = lens[...].astype(jnp.float32)
    game = lax.broadcasted_iota(jnp.int32, (games, games), 1).astype(jnp.float32)
    owned = owns[...] == trainer
    game_of = jnp.sum(jnp.where(owned, game, 0.0), axis=1, keepdims=True)
    held_len = jnp.sum(jnp.where(owned, length, 0.0), axis=1, keepdims=True)
    held_start = jnp.sum(jnp.where(game < game_of, length, 0.0), axis=1, keepdims=True)
    offset = lax.broadcasted_iota(jnp.int32, (games, rows), 1).astype(jnp.float32) - held_start
    usable = offset < held_len

    reward = rews[...]
    half = SIDE * FIELDS
    lane = lax.broadcasted_iota(jnp.int32, (games, LANES), 1) - to_y * FIELDS - jnp.where(near, 0, half)
    note = jnp.where(lane == CAP, held_len, 0.0)
    note = jnp.where(lane == CAP + 1, jnp.sum(reward), note)
    note = jnp.where(lane == CAP + 2, jnp.sum(reward * reward), note)
    chosen = []
    for j in range(CAP):
        chosen.append((offset == float(j)) & usable)
        held = jnp.sum(jnp.where(chosen[j], reward, 0.0), axis=1, keepdims=True)
        note = jnp.where(lane == j, held, note)
    crossing = jnp.zeros((SIDE, LANES), jnp.float32)
    for k in range(SIDE):
        note_z[k] = jnp.sum(note[k * SIDE : (k + 1) * SIDE], axis=0, keepdims=True)
        crossing = crossing + note[games // 2 + k * SIDE : games // 2 + (k + 1) * SIDE]
    note_c[...] = crossing.reshape(note_c.shape)

    inputs[0].wait()
    x = feats[...].astype(jnp.float32)
    square_mean = jnp.mean(x * x, axis=-1, keepdims=True)
    normed = (x * lax.rsqrt(square_mean + EPS_NORM) * gain[...]).astype(jnp.bfloat16)
    for j in range(CAP):
        picked = jnp.dot(
            chosen[j].astype(jnp.float32).astype(jnp.bfloat16), normed, preferred_element_type=jnp.float32
        )
        for t in range(games // 8):
            for q in range(tiles):
                wide[pl.ds(t * 8 * piece + j * tiles + q, 8, stride=piece), :] = picked[
                    t * 8 : t * 8 + 8, q * LANES : (q + 1) * LANES
                ]
    packed[...] = wide[...].astype(jnp.bfloat16).reshape(packed.shape)
    via_z[z] = packed[0, z]
    via_y[y] = packed[1, y]
    notes1[z] = note_z[z]

    pl.semaphore_wait(barrier, 3 * SIDE - 2 + n_rep - 1)

    def send(src, dst, send_sem, recv_sem, peer):
        pltpu.make_async_remote_copy(
            src_ref=src, dst_ref=dst, send_sem=send_sem, recv_sem=recv_sem, device_id=peer, device_id_type=MESH
        ).start()

    for k in Z_ORDER:

        @pl.when(k != z)
        def _():
            send(note_z.at[k], notes1.at[z], n1_send, n1_recv, {"actors": actor(y, k, c)})

        send(note_c.at[k], notes1.at[SIDE + z], n1_send, n1_recv, {"actors": actor(y, k, c + 1)})
    for to_z, to_y in zip(Z_ORDER, Y_ORDER):

        @pl.when(to_z != z)
        def _():
            send(packed.at[0, to_z], via_z.at[z], a_send, a_recv.at[z], {"actors": actor(y, to_z, c)})

        @pl.when(to_y != y)
        def _():
            send(packed.at[1, to_y], via_y.at[y], b_send, b_recv.at[y], {"actors": actor(to_y, z, c)})

    wait(n1_recv, notes1.at[pl.ds(1, 2 * SIDE - 1)])
    notes2[y] = notes1[0:SIDE] + notes1[SIDE:]
    for k in Y_ORDER:

        @pl.when(k != y)
        def _():
            send(notes2.at[y], notes2.at[y], n2_send, n2_recv, {"actors": actor(k, z, c)})

    here = {"y": 0, "z": 0}
    for at, (axis, (low, high), (first, last)) in enumerate(STEPS):
        via, arrived_at, mine_at = (via_z, a_recv, z) if axis == "y" else (via_y, b_recv, y)
        for k in range(here[axis], high):

            @pl.when(k != mine_at)
            def _():
                wait(arrived_at.at[k], via.at[k])

        here[axis] = max(here[axis], high)
        some = pl.ds(low, high - low)
        for k in Y_ORDER if axis == "y" else Z_ORDER:
            if not first <= k < last:
                continue
            if axis == "y":

                @pl.when(k != y)
                def _():
                    send(
                        via_z.at[some, k], land_z.at[y, some], a2_send, a2_recv.at[y, at],
                        {"actors": actor(k, z, c)},
                    )

            else:
                send(
                    via_y.at[some, k], land_y.at[z, some], b2_send, b2_recv.at[z, at],
                    {"actors": actor(y, k, c + 1)},
                )

    wait(n2_recv, notes2.at[pl.ds(1, SIDE - 1)])
    arrived = notes2[...].reshape(SIDE * SIDE, LANES)
    total = jnp.sum(arrived, axis=0, keepdims=True)
    mine[...] = total
    for k in range(1, n_rep):
        send(mine, others.at[k - 1], s_send.at[k - 1], s_recv.at[k - 1], {"rep": lax.rem(rep + k, n_rep)})

    def widen(value, from_y, from_z, core):
        source = actor(from_y, from_z, core)
        spread_rows[pl.ds(pl.multiple_of(source * piece, 8), piece), :] = value.astype(jnp.float32)

    for k in range(SIDE):
        widen(via_z[k, y], y, k, c)

    for k in range(1, n_rep):
        wait(s_recv.at[k - 1], others.at[k - 1])
    for k in range(1, n_rep):
        total = total + others[k - 1]
    row_lane = lax.broadcasted_iota(jnp.int32, (1, LANES), 1) - y * FIELDS

    def field(i):
        return jnp.sum(jnp.where((row_lane == i) | (row_lane == i + half), total, 0.0), axis=1, keepdims=True)

    counts[...] = jnp.broadcast_to(field(CAP), counts.shape).astype(jnp.int32)
    mean = field(CAP + 1) / row_total
    spread = lax.rsqrt(field(CAP + 2) / row_total - mean * mean + EPS_VAR)
    pair = lax.broadcasted_iota(jnp.int32, (SIDE * SIDE, 1), 0)
    slots = games * CAP
    lane = lax.broadcasted_iota(jnp.int32, (SIDE * SIDE, LANES), 1) - y * FIELDS

    def column(i):
        return jnp.sum(jnp.where(lane == i, arrived, 0.0), axis=1, keepdims=True)

    out = jnp.zeros((SIDE * SIDE, slots), jnp.float32)
    for h in range(2):
        source = pair * 2 + jnp.where(h == c, 0, 1)
        slot = lax.broadcasted_iota(jnp.int32, (SIDE * SIDE, slots), 1) - CAP * source
        held_len = column(h * half + CAP)
        for j in range(CAP):
            value = jnp.where(float(j) < held_len, (column(h * half + j) - mean) * spread, 0.0)
            out = out + jnp.where(slot == j, value, 0.0)
    spread_rews[...] = jnp.sum(out, axis=0, keepdims=True)

    for at, (axis, (low, high), (first, last)) in enumerate(STEPS):
        some = pl.ds(low, high - low)
        mine_at = y if axis == "y" else z

        @pl.when((mine_at >= first) & (mine_at < last))
        def _():
            for k in Y_ORDER if axis == "y" else Z_ORDER:
                if axis == "y":

                    @pl.when(k != y)
                    def _():
                        wait(a2_recv.at[k, at], land_z.at[k, some])
                        for i in range(low, high):
                            widen(land_z[k, i], k, i, c)

                else:
                    wait(b2_recv.at[k, at], land_y.at[k, some])
                    for i in range(low, high):
                        widen(land_y[k, i], i, k, c + 1)

    rest = pl.ds(1, SIDE - 1)
    wait(n1_send, notes1.at[pl.ds(1, 2 * SIDE - 1)])
    wait(n2_send, notes2.at[rest])
    for k in range(1, n_rep):
        wait(s_send.at[k - 1], others.at[k - 1])
    wait(a_send, via_z.at[rest])
    wait(b_send, via_y.at[rest])
    wait(a2_send, land_z.at[rest])
    wait(b2_send, land_y)


def write_kernel(spread_rows, spread_rews, count, rows, rews, counts):
    tiles = rows.shape[1] // LANES
    for r in range(rows.shape[0] // 8):
        for q in range(tiles):
            rows[r * 8 : r * 8 + 8, q * LANES : (q + 1) * LANES] = spread_rows[
                pl.ds(r * 8 * tiles + q, 8, stride=tiles), :
            ].astype(jnp.bfloat16)
    rews[...] = spread_rews[...]
    counts[0] = jnp.max(count[...])


def local(n, n_rep, features, rewards, lengths, owners, norm_gain):
    rows, width = features.shape[2:]
    games = lengths.shape[2]
    piece = CAP * width // LANES
    slots = games * CAP
    DMA = pltpu.SemaphoreType.DMA
    inputs = (features[0, 0], rewards[0], lengths[0], owners[0], norm_gain[None])
    block = pltpu.VMEM((SIDE, SIDE, piece, LANES), jnp.bfloat16)
    spread_rows, spread_rews, count = pl.pallas_call(
        functools.partial(route_kernel, n_rep, float(rows * n * n_rep)),
        out_shape=(
            jax.ShapeDtypeStruct((games * piece, LANES), jnp.float32),
            jax.ShapeDtypeStruct((1, slots), jnp.float32),
            jax.ShapeDtypeStruct((1, LANES), jnp.int32),
        ),
        in_specs=[HBM] * 5,
        out_specs=(VMEM,) * 3,
        scratch_shapes=[
            pltpu.VMEM((rows, width), jnp.bfloat16),
            pltpu.VMEM((1, rows), jnp.float32),
            pltpu.VMEM((1, games), jnp.int32),
            pltpu.VMEM((1, games), jnp.int32),
            pltpu.VMEM((1, width), jnp.float32),
            pltpu.VMEM((games * piece, LANES), jnp.float32),
            pltpu.VMEM((2, SIDE, SIDE, piece, LANES), jnp.bfloat16),
            block,
            block,
            block,
            block,
            pltpu.VMEM((SIDE, 1, LANES), jnp.float32),
            pltpu.VMEM((SIDE, 1, LANES), jnp.float32),
            pltpu.VMEM((2 * SIDE, 1, LANES), jnp.float32),
            pltpu.VMEM((SIDE, SIDE, 1, LANES), jnp.float32),
            pltpu.VMEM((1, LANES), jnp.float32),
            pltpu.VMEM((n_rep - 1, 1, LANES), jnp.float32),
            DMA((5,)),
            DMA,
            DMA,
            DMA((SIDE,)),
            DMA((SIDE,)),
            DMA,
            DMA,
            DMA((SIDE, len(STEPS))),
            DMA((SIDE, len(STEPS))),
            DMA,
            DMA,
            DMA,
            DMA,
            DMA((n_rep - 1,)),
            DMA((n_rep - 1,)),
        ],
        compiler_params=pltpu.CompilerParams(
            collective_id=0, has_side_effects=True, vmem_limit_bytes=24 * 1024 * 1024
        ),
        name="route",
    )(*(pltpu.with_memory_space_constraint(a, pltpu.HBM) for a in inputs))
    landed, scaled, counts = pl.pallas_call(
        write_kernel,
        out_shape=(
            jax.ShapeDtypeStruct((slots, width), jnp.bfloat16),
            jax.ShapeDtypeStruct((1, slots), jnp.float32),
            jax.ShapeDtypeStruct((1,), jnp.int32),
        ),
        in_specs=[VMEM] * 3,
        out_specs=(VMEM, VMEM, SMEM),
        compiler_params=pltpu.CompilerParams(vmem_limit_bytes=24 * 1024 * 1024),
        name="write",
    )(spread_rows, spread_rews, count)
    return landed.reshape(1, 1, slots, width), scaled.reshape(1, 1, slots), counts


def solution(mesh):
    n, n_rep = mesh.shape["actors"], mesh.shape["rep"]
    return jax.shard_map(
        functools.partial(local, n, n_rep),
        mesh=mesh,
        in_specs=(
            P("rep", "actors", None, None),
            P("rep", "actors", None),
            P("rep", "actors", None),
            P("rep", "actors", None),
            P(),
        ),
        out_specs=(P("rep", "actors", None, None), P("rep", "actors", None), P("actors")),
        check_vma=False,
    )
```

```python
import functools

import jax
import jax.numpy as jnp
from jax import lax
from jax.experimental import pallas as pl
from jax.experimental.pallas import tpu as pltpu
from jax.sharding import PartitionSpec as P

CAP = 3
EPS_NORM = 1e-06
EPS_VAR = 1e-05
LANES = 128
SIDE = 8
FIELDS = 8
Z_ORDER = (0, 1, 2, 3, 4, 5, 6, 7)
Y_ORDER = (0, 1, 2, 3, 7, 6, 5, 4)
STEPS = (('y', (0, 8), (0, 8)), ('z', (0, 8), (0, 8)))
VMEM = pl.BlockSpec(memory_space=pltpu.VMEM)
SMEM = pl.BlockSpec(memory_space=pltpu.SMEM)
HBM = pl.BlockSpec(memory_space=pltpu.HBM)
MESH = pl.DeviceIdType.MESH


def place():
    me = lax.axis_index("actors")
    return me // (2 * SIDE), lax.rem(me // 2, SIDE), lax.rem(me, 2)


def actor(y, z, c):
    return (lax.rem(y, SIDE) * SIDE + lax.rem(z, SIDE)) * 2 + lax.rem(c, 2)


def wait(sem, ref):
    pltpu.make_async_copy(ref, ref, sem).wait()


def route_kernel(
    n_rep, row_total, feats_in, rews_in, lens_in, owns_in, gain_in, spread_rows, spread_rews, counts,
    feats, rews, lens, owns, gain, wide, packed, via_z, via_y, land_z, land_y,
    note_z, note_c, notes1, notes2, mine, others,
    in_sem, a_send, b_send, a_recv, b_recv, a2_send, b2_send, a2_recv, b2_recv,
    n1_send, n1_recv, n2_send, n2_recv, s_send, s_recv,
):
    y, z, c = place()
    rep = lax.axis_index("rep")
    tiles = feats.shape[1] // LANES
    piece = CAP * tiles
    rows = feats.shape[0]
    games = lens.shape[1]

    inputs = [
        pltpu.make_async_copy(src, dst, in_sem.at[i])
        for i, (src, dst) in enumerate(
            ((feats_in, feats), (rews_in, rews), (lens_in, lens), (owns_in, owns), (gain_in, gain))
        )
    ]
    barrier = pltpu.get_barrier_semaphore()
    for d in (4, 5, 3, 6, 2, 7, 1):
        for peer in (actor(y, z + d, c), actor(y + d, z, c), actor(y, z + d, c + 1)):
            pl.semaphore_signal(barrier, inc=1, device_id={"actors": peer}, device_id_type=MESH)
    pl.semaphore_signal(barrier, inc=1, device_id={"actors": actor(y, z, c + 1)}, device_id_type=MESH)
    for k in range(1, n_rep):
        pl.semaphore_signal(barrier, inc=1, device_id={"rep": lax.rem(rep + k, n_rep)}, device_id_type=MESH)
    for copy in inputs:
        copy.start()
    for copy in inputs[1:]:
        copy.wait()

    row = lax.broadcasted_iota(jnp.int32, (games, 1), 0)
    inner = row & (SIDE - 1)
    step = (row // SIDE) & (SIDE - 1)
    near = row < games // 2
    to_y = jnp.where(near, inner, step)
    to_z = jnp.where(near, step, inner)
    trainer = (to_y * SIDE + to_z) * 2 + jnp.where(near, c, 1 - c)
    length = lens[...].astype(jnp.float32)
    game = lax.broadcasted_iota(jnp.int32, (games, games), 1).astype(jnp.float32)
    owned = owns[...] == trainer
    game_of = jnp.sum(jnp.where(owned, game, 0.0), axis=1, keepdims=True)
    held_len = jnp.sum(jnp.where(owned, length, 0.0), axis=1, keepdims=True)
    held_start = jnp.sum(jnp.where(game < game_of, length, 0.0), axis=1, keepdims=True)
    offset = lax.broadcasted_iota(jnp.int32, (games, rows), 1).astype(jnp.float32) - held_start
    usable = offset < held_len

    reward = rews[...]
    half = SIDE * FIELDS
    lane = lax.broadcasted_iota(jnp.int32, (games, LANES), 1) - to_y * FIELDS - jnp.where(near, 0, half)
    note = jnp.where(lane == CAP, held_len, 0.0)
    note = jnp.where(lane == CAP + 1, jnp.sum(reward), note)
    note = jnp.where(lane == CAP + 2, jnp.sum(reward * reward), note)
    chosen = []
    for j in range(CAP):
        chosen.append((offset == float(j)) & usable)
        held = jnp.sum(jnp.where(chosen[j], reward, 0.0), axis=1, keepdims=True)
        note = jnp.where(lane == j, held, note)
    crossing = jnp.zeros((SIDE, LANES), jnp.float32)
    for k in range(SIDE):
        note_z[k] = jnp.sum(note[k * SIDE : (k + 1) * SIDE], axis=0, keepdims=True)
        crossing = crossing + note[games // 2 + k * SIDE : games // 2 + (k + 1) * SIDE]
    note_c[...] = crossing.reshape(note_c.shape)

    inputs[0].wait()
    x = feats[...].astype(jnp.float32)
    square_mean = jnp.mean(x * x, axis=-1, keepdims=True)
    normed = (x * lax.rsqrt(square_mean + EPS_NORM) * gain[...]).astype(jnp.bfloat16)
    for j in range(CAP):
        picked = jnp.dot(
            chosen[j].astype(jnp.float32).astype(jnp.bfloat16), normed, preferred_element_type=jnp.float32
        )
        for t in range(games // 8):
            for q in range(tiles):
                wide[pl.ds(t * 8 * piece + j * tiles + q, 8, stride=piece), :] = picked[
                    t * 8 : t * 8 + 8, q * LANES : (q + 1) * LANES
                ]
    packed[...] = wide[...].astype(jnp.bfloat16).reshape(packed.shape)
    via_z[z] = packed[0, z]
    via_y[y] = packed[1, y]
    notes1[z] = note_z[z]

    pl.semaphore_wait(barrier, 3 * SIDE - 2 + n_rep - 1)

    def send(src, dst, send_sem, recv_sem, peer):
        pltpu.make_async_remote_copy(
            src_ref=src, dst_ref=dst, send_sem=send_sem, recv_sem=recv_sem, device_id=peer, device_id_type=MESH
        ).start()

    for k in Z_ORDER:

        @pl.when(k != z)
        def _():
            send(note_z.at[k], notes1.at[z], n1_send, n1_recv, {"actors": actor(y, k, c)})

        send(note_c.at[k], notes1.at[SIDE + z], n1_send, n1_recv, {"actors": actor(y, k, c + 1)})
    for to_z, to_y in zip(Z_ORDER, Y_ORDER):

        @pl.when(to_z != z)
        def _():
            send(packed.at[0, to_z], via_z.at[z], a_send, a_recv.at[z], {"actors": actor(y, to_z, c)})

        @pl.when(to_y != y)
        def _():
            send(packed.at[1, to_y], via_y.at[y], b_send, b_recv.at[y], {"actors": actor(to_y, z, c)})

    wait(n1_recv, notes1.at[pl.ds(1, 2 * SIDE - 1)])
    notes2[y] = notes1[0:SIDE] + notes1[SIDE:]
    for k in Y_ORDER:

        @pl.when(k != y)
        def _():
            send(notes2.at[y], notes2.at[y], n2_send, n2_recv, {"actors": actor(k, z, c)})

    here = {"y": 0, "z": 0}
    for at, (axis, (low, high), (first, last)) in enumerate(STEPS):
        via, arrived_at, mine_at = (via_z, a_recv, z) if axis == "y" else (via_y, b_recv, y)
        for k in range(here[axis], high):

            @pl.when(k != mine_at)
            def _():
                wait(arrived_at.at[k], via.at[k])

        here[axis] = max(here[axis], high)
        some = pl.ds(low, high - low)
        for k in Y_ORDER if axis == "y" else Z_ORDER:
            if not first <= k < last:
                continue
            if axis == "y":

                @pl.when(k != y)
                def _():
                    send(
                        via_z.at[some, k], land_z.at[y, some], a2_send, a2_recv.at[y, at],
                        {"actors": actor(k, z, c)},
                    )

            else:
                send(
                    via_y.at[some, k], land_y.at[z, some], b2_send, b2_recv.at[z, at],
                    {"actors": actor(y, k, c + 1)},
                )

    wait(n2_recv, notes2.at[pl.ds(1, SIDE - 1)])
    arrived = notes2[...].reshape(SIDE * SIDE, LANES)
    total = jnp.sum(arrived, axis=0, keepdims=True)
    mine[...] = total
    for k in range(1, n_rep):
        send(mine, others.at[k - 1], s_send.at[k - 1], s_recv.at[k - 1], {"rep": lax.rem(rep + k, n_rep)})

    def widen(value, from_y, from_z, core):
        source = actor(from_y, from_z, core)
        spread_rows[pl.ds(pl.multiple_of(source * piece, 8), piece), :] = value.astype(jnp.float32)

    for k in range(SIDE):
        widen(via_z[k, y], y, k, c)

    for k in range(1, n_rep):
        wait(s_recv.at[k - 1], others.at[k - 1])
    for k in range(1, n_rep):
        total = total + others[k - 1]
    row_lane = lax.broadcasted_iota(jnp.int32, (1, LANES), 1) - y * FIELDS

    def field(i):
        return jnp.sum(jnp.where((row_lane == i) | (row_lane == i + half), total, 0.0), axis=1, keepdims=True)

    counts[...] = jnp.broadcast_to(field(CAP), counts.shape).astype(jnp.int32)
    mean = field(CAP + 1) / row_total
    spread = lax.rsqrt(field(CAP + 2) / row_total - mean * mean + EPS_VAR)
    pair = lax.broadcasted_iota(jnp.int32, (SIDE * SIDE, 1), 0)
    slots = games * CAP
    lane = lax.broadcasted_iota(jnp.int32, (SIDE * SIDE, LANES), 1) - y * FIELDS

    def column(i):
        return jnp.sum(jnp.where(lane == i, arrived, 0.0), axis=1, keepdims=True)

    out = jnp.zeros((SIDE * SIDE, slots), jnp.float32)
    for h in range(2):
        source = pair * 2 + jnp.where(h == c, 0, 1)
        slot = lax.broadcasted_iota(jnp.int32, (SIDE * SIDE, slots), 1) - CAP * source
        held_len = column(h * half + CAP)
        for j in range(CAP):
            value = jnp.where(float(j) < held_len, (column(h * half + j) - mean) * spread, 0.0)
            out = out + jnp.where(slot == j, value, 0.0)
    spread_rews[...] = jnp.sum(out, axis=0, keepdims=True)

    for at, (axis, (low, high), (first, last)) in enumerate(STEPS):
        some = pl.ds(low, high - low)
        mine_at = y if axis == "y" else z

        @pl.when((mine_at >= first) & (mine_at < last))
        def _():
            for k in Y_ORDER if axis == "y" else Z_ORDER:
                if axis == "y":

                    @pl.when(k != y)
                    def _():
                        wait(a2_recv.at[k, at], land_z.at[k, some])
                        for i in range(low, high):
                            widen(land_z[k, i], k, i, c)

                else:
                    wait(b2_recv.at[k, at], land_y.at[k, some])
                    for i in range(low, high):
                        widen(land_y[k, i], i, k, c + 1)

    rest = pl.ds(1, SIDE - 1)
    wait(n1_send, notes1.at[pl.ds(1, 2 * SIDE - 1)])
    wait(n2_send, notes2.at[rest])
    for k in range(1, n_rep):
        wait(s_send.at[k - 1], others.at[k - 1])
    wait(a_send, via_z.at[rest])
    wait(b_send, via_y.at[rest])
    wait(a2_send, land_z.at[rest])
    wait(b2_send, land_y)


def write_kernel(spread_rows, spread_rews, count, rows, rews, counts):
    tiles = rows.shape[1] // LANES
    for r in range(rows.shape[0] // 8):
        for q in range(tiles):
            rows[r * 8 : r * 8 + 8, q * LANES : (q + 1) * LANES] = spread_rows[
                pl.ds(r * 8 * tiles + q, 8, stride=tiles), :
            ].astype(jnp.bfloat16)
    rews[...] = spread_rews[...]
    counts[0] = jnp.max(count[...])


def local(n, n_rep, features, rewards, lengths, owners, norm_gain):
    rows, width = features.shape[2:]
    games = lengths.shape[2]
    piece = CAP * width // LANES
    slots = games * CAP
    DMA = pltpu.SemaphoreType.DMA
    inputs = (features[0, 0], rewards[0], lengths[0], owners[0], norm_gain[None])
    block = pltpu.VMEM((SIDE, SIDE, piece, LANES), jnp.bfloat16)
    spread_rows, spread_rews, count = pl.pallas_call(
        functools.partial(route_kernel, n_rep, float(rows * n * n_rep)),
        out_shape=(
            jax.ShapeDtypeStruct((games * piece, LANES), jnp.float32),
            jax.ShapeDtypeStruct((1, slots), jnp.float32),
            jax.ShapeDtypeStruct((1, LANES), jnp.int32),
        ),
        in_specs=[HBM] * 5,
        out_specs=(VMEM,) * 3,
        scratch_shapes=[
            pltpu.VMEM((rows, width), jnp.bfloat16),
            pltpu.VMEM((1, rows), jnp.float32),
            pltpu.VMEM((1, games), jnp.int32),
            pltpu.VMEM((1, games), jnp.int32),
            pltpu.VMEM((1, width), jnp.float32),
            pltpu.VMEM((games * piece, LANES), jnp.float32),
            pltpu.VMEM((2, SIDE, SIDE, piece, LANES), jnp.bfloat16),
            block,
            block,
            block,
            block,
            pltpu.VMEM((SIDE, 1, LANES), jnp.float32),
            pltpu.VMEM((SIDE, 1, LANES), jnp.float32),
            pltpu.VMEM((2 * SIDE, 1, LANES), jnp.float32),
            pltpu.VMEM((SIDE, SIDE, 1, LANES), jnp.float32),
            pltpu.VMEM((1, LANES), jnp.float32),
            pltpu.VMEM((n_rep - 1, 1, LANES), jnp.float32),
            DMA((5,)),
            DMA,
            DMA,
            DMA((SIDE,)),
            DMA((SIDE,)),
            DMA,
            DMA,
            DMA((SIDE, len(STEPS))),
            DMA((SIDE, len(STEPS))),
            DMA,
            DMA,
            DMA,
            DMA,
            DMA((n_rep - 1,)),
            DMA((n_rep - 1,)),
        ],
        compiler_params=pltpu.CompilerParams(
            collective_id=0, has_side_effects=True, vmem_limit_bytes=24 * 1024 * 1024
        ),
        name="route",
    )(*(pltpu.with_memory_space_constraint(a, pltpu.HBM) for a in inputs))
    landed, scaled, counts = pl.pallas_call(
        write_kernel,
        out_shape=(
            jax.ShapeDtypeStruct((slots, width), jnp.bfloat16),
            jax.ShapeDtypeStruct((1, slots), jnp.float32),
            jax.ShapeDtypeStruct((1,), jnp.int32),
        ),
        in_specs=[VMEM] * 3,
        out_specs=(VMEM, VMEM, SMEM),
        compiler_params=pltpu.CompilerParams(vmem_limit_bytes=24 * 1024 * 1024),
        name="write",
    )(spread_rows, spread_rews, count)
    return landed.reshape(1, 1, slots, width), scaled.reshape(1, 1, slots), counts


def solution(mesh):
    n, n_rep = mesh.shape["actors"], mesh.shape["rep"]
    return jax.shard_map(
        functools.partial(local, n, n_rep),
        mesh=mesh,
        in_specs=(
            P("rep", "actors", None, None),
            P("rep", "actors", None),
            P("rep", "actors", None),
            P("rep", "actors", None),
            P(),
        ),
        out_specs=(P("rep", "actors", None, None), P("rep", "actors", None), P("actors")),
        check_vma=False,
    )
```

```python
import functools

import jax
import jax.numpy as jnp
from jax import lax
from jax.experimental import pallas as pl
from jax.experimental.pallas import tpu as pltpu
from jax.sharding import PartitionSpec as P

CAP = 3
EPS_NORM = 1e-06
EPS_VAR = 1e-05
LANES = 128
SIDE = 8
FIELDS = 8
Z_ORDER = (0, 1, 2, 3, 4, 5, 6, 7)
Y_ORDER = (0, 1, 2, 3, 7, 6, 5, 4)
STEPS = (('y', (0, 8), (0, 8)), ('z', (0, 8), (0, 8)))
VMEM = pl.BlockSpec(memory_space=pltpu.VMEM)
SMEM = pl.BlockSpec(memory_space=pltpu.SMEM)
HBM = pl.BlockSpec(memory_space=pltpu.HBM)
MESH = pl.DeviceIdType.MESH


def place():
    me = lax.axis_index("actors")
    return me // (2 * SIDE), lax.rem(me // 2, SIDE), lax.rem(me, 2)


def actor(y, z, c):
    return (lax.rem(y, SIDE) * SIDE + lax.rem(z, SIDE)) * 2 + lax.rem(c, 2)


def y_turns(y):
    half = SIDE // 2
    return [part + lax.rem(y + i, half) for part in (0, half) for i in range(half)]


def wait(sem, ref):
    pltpu.make_async_copy(ref, ref, sem).wait()


def route_kernel(
    n_rep, row_total, feats_in, rews_in, lens_in, owns_in, gain_in, spread_rows, spread_rews, counts,
    feats, rews, lens, owns, gain, wide, packed, via_z, via_y, land_z, land_y,
    note_z, note_c, notes1, notes2, mine, others,
    in_sem, a_send, b_send, a_recv, b_recv, a2_send, b2_send, a2_recv, b2_recv,
    n1_send, n1_recv, n2_send, n2_recv, s_send, s_recv,
):
    y, z, c = place()
    rep = lax.axis_index("rep")
    tiles = feats.shape[1] // LANES
    piece = CAP * tiles
    rows = feats.shape[0]
    games = lens.shape[1]

    inputs = [
        pltpu.make_async_copy(src, dst, in_sem.at[i])
        for i, (src, dst) in enumerate(
            ((feats_in, feats), (rews_in, rews), (lens_in, lens), (owns_in, owns), (gain_in, gain))
        )
    ]
    barrier = pltpu.get_barrier_semaphore()
    for d in (4, 5, 3, 6, 2, 7, 1):
        for peer in (actor(y, z + d, c), actor(y + d, z, c), actor(y, z + d, c + 1)):
            pl.semaphore_signal(barrier, inc=1, device_id={"actors": peer}, device_id_type=MESH)
    pl.semaphore_signal(barrier, inc=1, device_id={"actors": actor(y, z, c + 1)}, device_id_type=MESH)
    for k in range(1, n_rep):
        pl.semaphore_signal(barrier, inc=1, device_id={"rep": lax.rem(rep + k, n_rep)}, device_id_type=MESH)
    for copy in inputs:
        copy.start()
    for copy in inputs[1:]:
        copy.wait()

    row = lax.broadcasted_iota(jnp.int32, (games, 1), 0)
    inner = row & (SIDE - 1)
    step = (row // SIDE) & (SIDE - 1)
    near = row < games // 2
    to_y = jnp.where(near, inner, step)
    to_z = jnp.where(near, step, inner)
    trainer = (to_y * SIDE + to_z) * 2 + jnp.where(near, c, 1 - c)
    length = lens[...].astype(jnp.float32)
    game = lax.broadcasted_iota(jnp.int32, (games, games), 1).astype(jnp.float32)
    owned = owns[...] == trainer
    game_of = jnp.sum(jnp.where(owned, game, 0.0), axis=1, keepdims=True)
    held_len = jnp.sum(jnp.where(owned, length, 0.0), axis=1, keepdims=True)
    held_start = jnp.sum(jnp.where(game < game_of, length, 0.0), axis=1, keepdims=True)
    offset = lax.broadcasted_iota(jnp.int32, (games, rows), 1).astype(jnp.float32) - held_start
    usable = offset < held_len

    reward = rews[...]
    half = SIDE * FIELDS
    lane = lax.broadcasted_iota(jnp.int32, (games, LANES), 1) - to_y * FIELDS - jnp.where(near, 0, half)
    note = jnp.where(lane == CAP, held_len, 0.0)
    note = jnp.where(lane == CAP + 1, jnp.sum(reward), note)
    note = jnp.where(lane == CAP + 2, jnp.sum(reward * reward), note)
    chosen = []
    for j in range(CAP):
        chosen.append((offset == float(j)) & usable)
        held = jnp.sum(jnp.where(chosen[j], reward, 0.0), axis=1, keepdims=True)
        note = jnp.where(lane == j, held, note)
    crossing = jnp.zeros((SIDE, LANES), jnp.float32)
    for k in range(SIDE):
        note_z[k] = jnp.sum(note[k * SIDE : (k + 1) * SIDE], axis=0, keepdims=True)
        crossing = crossing + note[games // 2 + k * SIDE : games // 2 + (k + 1) * SIDE]
    note_c[...] = crossing.reshape(note_c.shape)

    inputs[0].wait()
    x = feats[...].astype(jnp.float32)
    square_mean = jnp.mean(x * x, axis=-1, keepdims=True)
    normed = (x * lax.rsqrt(square_mean + EPS_NORM) * gain[...]).astype(jnp.bfloat16)
    for j in range(CAP):
        picked = jnp.dot(
            chosen[j].astype(jnp.float32).astype(jnp.bfloat16), normed, preferred_element_type=jnp.float32
        )
        for t in range(games // 8):
            for q in range(tiles):
                wide[pl.ds(t * 8 * piece + j * tiles + q, 8, stride=piece), :] = picked[
                    t * 8 : t * 8 + 8, q * LANES : (q + 1) * LANES
                ]
    packed[...] = wide[...].astype(jnp.bfloat16).reshape(packed.shape)
    via_z[z] = packed[0, z]
    via_y[y] = packed[1, y]
    notes1[z] = note_z[z]

    pl.semaphore_wait(barrier, 3 * SIDE - 2 + n_rep - 1)

    def send(src, dst, send_sem, recv_sem, peer):
        pltpu.make_async_remote_copy(
            src_ref=src, dst_ref=dst, send_sem=send_sem, recv_sem=recv_sem, device_id=peer, device_id_type=MESH
        ).start()

    for k in Z_ORDER[::-1]:

        @pl.when(k != z)
        def _():
            send(note_z.at[k], notes1.at[z], n1_send, n1_recv, {"actors": actor(y, k, c)})

        send(note_c.at[k], notes1.at[SIDE + z], n1_send, n1_recv, {"actors": actor(y, k, c + 1)})
    for to_z, to_y in zip(Z_ORDER, y_turns(y)):

        @pl.when(to_z != z)
        def _():
            send(packed.at[0, to_z], via_z.at[z], a_send, a_recv.at[z], {"actors": actor(y, to_z, c)})

        @pl.when(to_y != y)
        def _():
            send(packed.at[1, to_y], via_y.at[y], b_send, b_recv.at[y], {"actors": actor(to_y, z, c)})

    wait(n1_recv, notes1.at[pl.ds(1, 2 * SIDE - 1)])
    notes2[y] = notes1[0:SIDE] + notes1[SIDE:]
    for k in Y_ORDER:

        @pl.when(k != y)
        def _():
            send(notes2.at[y], notes2.at[y], n2_send, n2_recv, {"actors": actor(k, z, c)})

    here = {"y": 0, "z": 0}
    for at, (axis, (low, high), (first, last)) in enumerate(STEPS):
        via, arrived_at, mine_at = (via_z, a_recv, z) if axis == "y" else (via_y, b_recv, y)
        for k in range(here[axis], high):

            @pl.when(k != mine_at)
            def _():
                wait(arrived_at.at[k], via.at[k])

        here[axis] = max(here[axis], high)
        some = pl.ds(low, high - low)
        for k in y_turns(y) if axis == "y" else Z_ORDER:
            if axis == "y":

                @pl.when(k != y)
                def _():
                    send(
                        via_z.at[some, k], land_z.at[y, some], a2_send, a2_recv.at[y, at],
                        {"actors": actor(k, z, c)},
                    )

            else:
                send(
                    via_y.at[some, k], land_y.at[z, some], b2_send, b2_recv.at[z, at],
                    {"actors": actor(y, k, c + 1)},
                )

    wait(n2_recv, notes2.at[pl.ds(1, SIDE - 1)])
    arrived = notes2[...].reshape(SIDE * SIDE, LANES)
    total = jnp.sum(arrived, axis=0, keepdims=True)
    mine[...] = total
    for k in range(1, n_rep):
        send(mine, others.at[k - 1], s_send.at[k - 1], s_recv.at[k - 1], {"rep": lax.rem(rep + k, n_rep)})

    def widen(value, from_y, from_z, core):
        source = actor(from_y, from_z, core)
        spread_rows[pl.ds(pl.multiple_of(source * piece, 8), piece), :] = value.astype(jnp.float32)

    for k in range(SIDE):
        widen(via_z[k, y], y, k, c)

    for k in range(1, n_rep):
        wait(s_recv.at[k - 1], others.at[k - 1])
    for k in range(1, n_rep):
        total = total + others[k - 1]
    row_lane = lax.broadcasted_iota(jnp.int32, (1, LANES), 1) - y * FIELDS

    def field(i):
        return jnp.sum(jnp.where((row_lane == i) | (row_lane == i + half), total, 0.0), axis=1, keepdims=True)

    counts[...] = jnp.broadcast_to(field(CAP), counts.shape).astype(jnp.int32)
    mean = field(CAP + 1) / row_total
    spread = lax.rsqrt(field(CAP + 2) / row_total - mean * mean + EPS_VAR)
    pair = lax.broadcasted_iota(jnp.int32, (SIDE * SIDE, 1), 0)
    slots = games * CAP
    lane = lax.broadcasted_iota(jnp.int32, (SIDE * SIDE, LANES), 1) - y * FIELDS

    def column(i):
        return jnp.sum(jnp.where(lane == i, arrived, 0.0), axis=1, keepdims=True)

    out = jnp.zeros((SIDE * SIDE, slots), jnp.float32)
    for h in range(2):
        source = pair * 2 + jnp.where(h == c, 0, 1)
        slot = lax.broadcasted_iota(jnp.int32, (SIDE * SIDE, slots), 1) - CAP * source
        held_len = column(h * half + CAP)
        for j in range(CAP):
            value = jnp.where(float(j) < held_len, (column(h * half + j) - mean) * spread, 0.0)
            out = out + jnp.where(slot == j, value, 0.0)
    spread_rews[...] = jnp.sum(out, axis=0, keepdims=True)

    for at, (axis, (low, high), (first, last)) in enumerate(STEPS):
        some = pl.ds(low, high - low)
        mine_at = y if axis == "y" else z

        @pl.when((mine_at >= first) & (mine_at < last))
        def _():
            for k in Y_ORDER if axis == "y" else Z_ORDER:
                if axis == "y":

                    @pl.when(k != y)
                    def _():
                        wait(a2_recv.at[k, at], land_z.at[k, some])
                        for i in range(low, high):
                            widen(land_z[k, i], k, i, c)

                else:
                    wait(b2_recv.at[k, at], land_y.at[k, some])
                    for i in range(low, high):
                        widen(land_y[k, i], i, k, c + 1)

    rest = pl.ds(1, SIDE - 1)
    wait(n1_send, notes1.at[pl.ds(1, 2 * SIDE - 1)])
    wait(n2_send, notes2.at[rest])
    for k in range(1, n_rep):
        wait(s_send.at[k - 1], others.at[k - 1])
    wait(a_send, via_z.at[rest])
    wait(b_send, via_y.at[rest])
    wait(a2_send, land_z.at[rest])
    wait(b2_send, land_y)


def write_kernel(spread_rows, spread_rews, count, rows, rews, counts):
    tiles = rows.shape[1] // LANES
    for r in range(rows.shape[0] // 8):
        for q in range(tiles):
            rows[r * 8 : r * 8 + 8, q * LANES : (q + 1) * LANES] = spread_rows[
                pl.ds(r * 8 * tiles + q, 8, stride=tiles), :
            ].astype(jnp.bfloat16)
    rews[...] = spread_rews[...]
    counts[0] = jnp.max(count[...])


def local(n, n_rep, features, rewards, lengths, owners, norm_gain):
    rows, width = features.shape[2:]
    games = lengths.shape[2]
    piece = CAP * width // LANES
    slots = games * CAP
    DMA = pltpu.SemaphoreType.DMA
    inputs = (features[0, 0], rewards[0], lengths[0], owners[0], norm_gain[None])
    block = pltpu.VMEM((SIDE, SIDE, piece, LANES), jnp.bfloat16)
    spread_rows, spread_rews, count = pl.pallas_call(
        functools.partial(route_kernel, n_rep, float(rows * n * n_rep)),
        out_shape=(
            jax.ShapeDtypeStruct((games * piece, LANES), jnp.float32),
            jax.ShapeDtypeStruct((1, slots), jnp.float32),
            jax.ShapeDtypeStruct((1, LANES), jnp.int32),
        ),
        in_specs=[HBM] * 5,
        out_specs=(VMEM,) * 3,
        scratch_shapes=[
            pltpu.VMEM((rows, width), jnp.bfloat16),
            pltpu.VMEM((1, rows), jnp.float32),
            pltpu.VMEM((1, games), jnp.int32),
            pltpu.VMEM((1, games), jnp.int32),
            pltpu.VMEM((1, width), jnp.float32),
            pltpu.VMEM((games * piece, LANES), jnp.float32),
            pltpu.VMEM((2, SIDE, SIDE, piece, LANES), jnp.bfloat16),
            block,
            block,
            block,
            block,
            pltpu.VMEM((SIDE, 1, LANES), jnp.float32),
            pltpu.VMEM((SIDE, 1, LANES), jnp.float32),
            pltpu.VMEM((2 * SIDE, 1, LANES), jnp.float32),
            pltpu.VMEM((SIDE, SIDE, 1, LANES), jnp.float32),
            pltpu.VMEM((1, LANES), jnp.float32),
            pltpu.VMEM((n_rep - 1, 1, LANES), jnp.float32),
            DMA((5,)),
            DMA,
            DMA,
            DMA((SIDE,)),
            DMA((SIDE,)),
            DMA,
            DMA,
            DMA((SIDE, len(STEPS))),
            DMA((SIDE, len(STEPS))),
            DMA,
            DMA,
            DMA,
            DMA,
            DMA((n_rep - 1,)),
            DMA((n_rep - 1,)),
        ],
        compiler_params=pltpu.CompilerParams(
            collective_id=0, has_side_effects=True, vmem_limit_bytes=24 * 1024 * 1024
        ),
        name="route",
    )(*(pltpu.with_memory_space_constraint(a, pltpu.HBM) for a in inputs))
    landed, scaled, counts = pl.pallas_call(
        write_kernel,
        out_shape=(
            jax.ShapeDtypeStruct((slots, width), jnp.bfloat16),
            jax.ShapeDtypeStruct((1, slots), jnp.float32),
            jax.ShapeDtypeStruct((1,), jnp.int32),
        ),
        in_specs=[VMEM] * 3,
        out_specs=(VMEM, VMEM, SMEM),
        compiler_params=pltpu.CompilerParams(vmem_limit_bytes=24 * 1024 * 1024),
        name="write",
    )(spread_rows, spread_rews, count)
    return landed.reshape(1, 1, slots, width), scaled.reshape(1, 1, slots), counts


def solution(mesh):
    n, n_rep = mesh.shape["actors"], mesh.shape["rep"]
    return jax.shard_map(
        functools.partial(local, n, n_rep),
        mesh=mesh,
        in_specs=(
            P("rep", "actors", None, None),
            P("rep", "actors", None),
            P("rep", "actors", None),
            P("rep", "actors", None),
            P(),
        ),
        out_specs=(P("rep", "actors", None, None), P("rep", "actors", None), P("actors")),
        check_vma=False,
    )
```
